32 devices in a mesh: fsdp: 32 (over z, y, x, core).
Axes of the slice: x: 2, y: 2, z: 4, core: 2. Of those that a mesh axis runs over, the one named last changes fastest.
Arguments:
- tokens: int32 [1024, 2], P('fsdp')
- positions: int32 [1024], P('fsdp')
- src_len: int32 [1024], P('fsdp')
- self_k: bfloat16 [2, 1024, 32, 16, 64], P(None, 'fsdp')
- self_v: bfloat16 [2, 1024, 32, 16, 64], P(None, 'fsdp')
- cross_k: bfloat16 [2, 1024, 32, 16, 64], P(None, 'fsdp')
- cross_v: bfloat16 [2, 1024, 32, 16, 64], P(None, 'fsdp')
- attn_w: bfloat16 [2, 6, 1024, 1024], P(None, None, 'fsdp')
- attn_b: bfloat16 [2, 6, 1024], P(None, None, 'fsdp')
- fc1_w: bfloat16 [2, 1024, 4096], P(None, 'fsdp')
- fc1_b: bfloat16 [2, 4096], P(None, 'fsdp')
- fc2_w: bfloat16 [2, 4096, 1024], P(None, 'fsdp')
- fc2_b: bfloat16 [2, 1024], P(None, 'fsdp')
- ln_gain: bfloat16 [2, 3, 1024], P(None, None, 'fsdp')
- ln_bias: bfloat16 [2, 3, 1024], P(None, None, 'fsdp')
- tok_embed: bfloat16 [50304, 1024], P('fsdp')
- pos_embed: bfloat16 [1026, 1024], replicated
- emb_norm: bfloat16 [2, 1024], replicated
- logit_bias: float32 [50304], P('fsdp')
Outputs:
- output 1: float32 [2, 1024, 50304], P(None, None, 'fsdp')
- output 2: bfloat16 [2, 1024, 32, 16, 64], P(None, 'fsdp')
- output 3: bfloat16 [2, 1024, 32, 16, 64], P(None, 'fsdp')
All inputs are finite; a program needn't handle non-finite values.
Results may differ from the reference program's by a relative error of at most 0.00767352.
Values are sent between devices in bfloat16 or wider.
A program may use at most 1 GiB of HBM per device.

```python
import jax
import jax.numpy as jnp
from jax import lax

D = 1024
HEADS = 16
FF = 4096
VOCAB = 50264
VOCAB_PAD = 50304
POS_ROWS = 1026
LAYERS = 2
STEPS = 2
BATCH = 1024
TMAX = 32
SRC = 32

HEAD_DIM = D // HEADS
LN_EPS = 1e-5


def draw_indices(base_key):
    key_tok, key_tpick, key_pos, key_ppick, key_src, key_spick = jax.random.split(base_key, 6)
    flat_ids = jnp.arange(BATCH * STEPS).reshape(BATCH, STEPS)
    tokens = jax.random.randint(key_tok, (BATCH, STEPS), 0, VOCAB)
    tokens = jnp.where(flat_ids == jax.random.randint(key_tpick, (), 0, BATCH * STEPS), VOCAB - 1, tokens)
    row_ids = jnp.arange(BATCH)
    positions = jax.random.randint(key_pos, (BATCH,), 0, TMAX - 1)
    positions = jnp.where(row_ids == jax.random.randint(key_ppick, (), 0, BATCH), TMAX - 2, positions)
    src_len = jax.random.randint(key_src, (BATCH,), 1, SRC + 1)
    src_len = jnp.where(row_ids == jax.random.randint(key_spick, (), 0, BATCH), SRC, src_len)
    return tokens.astype(jnp.int32), positions.astype(jnp.int32), src_len.astype(jnp.int32)


def setup_inputs(seed: int = 0) -> dict:
    key_idx, key_vals = jax.random.split(jax.random.key(seed))
    tokens, positions, src_len = draw_indices(key_idx)
    subkeys = jax.random.split(key_vals, 20)

    def normal(sub_key, out_shape, std_scale):
        return jax.random.normal(sub_key, out_shape, jnp.float32) * std_scale

    cache_shape = (LAYERS, BATCH, TMAX, HEADS, HEAD_DIM)
    cross_shape = (LAYERS, BATCH, SRC, HEADS, HEAD_DIM)
    slot_scale = jnp.array([1.0, 1.0, 1.0, 2.0, 1.0, 2.0], jnp.float32)[None, :, None, None] * D ** -0.5
    vocab_ids = jnp.arange(VOCAB_PAD)
    bias_real = normal(subkeys[17], (VOCAB_PAD,), 0.5)
    bias_pad = jax.random.uniform(subkeys[18], (VOCAB_PAD,), jnp.float32, -12.0, -8.0)
    emb_gain = 1.0 + normal(subkeys[15], (D,), 0.3)
    emb_shift = normal(subkeys[16], (D,), 0.3)
    return {
        'tokens': tokens,
        'positions': positions,
        'src_len': src_len,
        'self_k': normal(subkeys[0], cache_shape, 1.5).astype(jnp.bfloat16),
        'self_v': normal(subkeys[1], cache_shape, 1.0).astype(jnp.bfloat16),
        'cross_k': normal(subkeys[2], cross_shape, 1.5).astype(jnp.bfloat16),
        'cross_v': normal(subkeys[3], cross_shape, 1.0).astype(jnp.bfloat16),
        'attn_w': (normal(subkeys[4], (LAYERS, 6, D, D), 1.0) * slot_scale).astype(jnp.bfloat16),
        'attn_b': normal(subkeys[5], (LAYERS, 6, D), 0.3).astype(jnp.bfloat16),
        'fc1_w': normal(subkeys[6], (LAYERS, D, FF), D ** -0.5).astype(jnp.bfloat16),
        'fc1_b': normal(subkeys[7], (LAYERS, FF), 0.5).astype(jnp.bfloat16),
        'fc2_w': normal(subkeys[8], (LAYERS, FF, D), FF ** -0.5).astype(jnp.bfloat16),
        'fc2_b': normal(subkeys[9], (LAYERS, D), 0.3).astype(jnp.bfloat16),
        'ln_gain': (1.0 + normal(subkeys[10], (LAYERS, 3, D), 0.3)).astype(jnp.bfloat16),
        'ln_bias': normal(subkeys[11], (LAYERS, 3, D), 0.3).astype(jnp.bfloat16),
        'tok_embed': normal(subkeys[12], (VOCAB_PAD, D), D ** -0.5).astype(jnp.bfloat16),
        'pos_embed': normal(subkeys[13], (POS_ROWS, D), D ** -0.5).astype(jnp.bfloat16),
        'emb_norm': jnp.stack([emb_gain, emb_shift]).astype(jnp.bfloat16),
        'logit_bias': jnp.where(vocab_ids < VOCAB, bias_real, bias_pad),
    }


def layer_norm(values, gain_row, shift_row):
    row_mean = values.mean(-1, keepdims=True)
    centered = values - row_mean
    variance = (centered * centered).mean(-1, keepdims=True)
    return centered * lax.rsqrt(variance + LN_EPS) * gain_row.astype(jnp.float32) + shift_row.astype(jnp.float32)


def attend_one(operands):
    query_rows, key_rows, val_rows, valid_len = operands
    scores = jnp.einsum('hd,thd->ht', query_rows.astype(jnp.float32), key_rows.astype(jnp.float32))
    valid_mask = jnp.arange(key_rows.shape[0])[None, :] < valid_len
    scores = jnp.where(valid_mask, scores, -jnp.inf)
    weights = jnp.exp(scores - scores.max(-1, keepdims=True))
    weight_sum = weights.sum(-1, keepdims=True)
    mixed_rows = jnp.einsum('ht,thd->hd', weights.astype(jnp.bfloat16).astype(jnp.float32), val_rows.astype(jnp.float32))
    return mixed_rows / weight_sum


def project(act_rows, weight, bias_row):
    return jnp.dot(act_rows, weight, preferred_element_type=jnp.float32) + bias_row.astype(jnp.float32)


def reference(tokens, positions, src_len, self_k, self_v, cross_k, cross_v, attn_w, attn_b, fc1_w, fc1_b, fc2_w, fc2_b, ln_gain, ln_bias, tok_embed, pos_embed, emb_norm, logit_bias):
    attn_scale = HEAD_DIM ** -0.5
    time_ids = jnp.arange(TMAX)
    cache_k = [self_k[layer_idx] for layer_idx in range(LAYERS)]
    cache_v = [self_v[layer_idx] for layer_idx in range(LAYERS)]
    step_logits = []
    for step_idx in range(STEPS):
        step_pos = positions + step_idx
        start_rows = tok_embed[tokens[:, step_idx]].astype(jnp.float32) + pos_embed[step_pos + 2].astype(jnp.float32)
        hidden = layer_norm(start_rows, emb_norm[0], emb_norm[1])
        write_mask = (time_ids[None, :] == step_pos[:, None])[:, :, None, None]
        for layer_idx in range(LAYERS):
            layer_w = attn_w[layer_idx]
            layer_b = attn_b[layer_idx]
            act_rows = hidden.astype(jnp.bfloat16)
            self_query = (project(act_rows, layer_w[0], layer_b[0]) * attn_scale).astype(jnp.bfloat16).reshape(BATCH, HEADS, HEAD_DIM)
            new_key = project(act_rows, layer_w[1], layer_b[1]).astype(jnp.bfloat16).reshape(BATCH, 1, HEADS, HEAD_DIM)
            new_val = project(act_rows, layer_w[2], layer_b[2]).astype(jnp.bfloat16).reshape(BATCH, 1, HEADS, HEAD_DIM)
            cache_k[layer_idx] = jnp.where(write_mask, new_key, cache_k[layer_idx])
            cache_v[layer_idx] = jnp.where(write_mask, new_val, cache_v[layer_idx])
            mixed_rows = lax.map(attend_one, (self_query, cache_k[layer_idx], cache_v[layer_idx], step_pos + 1))
            attn_out = project(mixed_rows.reshape(BATCH, D).astype(jnp.bfloat16), layer_w[3], layer_b[3])
            hidden = layer_norm(hidden + attn_out, ln_gain[layer_idx, 0], ln_bias[layer_idx, 0])
            cross_query = (project(hidden.astype(jnp.bfloat16), layer_w[4], layer_b[4]) * attn_scale).astype(jnp.bfloat16).reshape(BATCH, HEADS, HEAD_DIM)
            mixed_rows = lax.map(attend_one, (cross_query, cross_k[layer_idx], cross_v[layer_idx], src_len))
            cross_out = project(mixed_rows.reshape(BATCH, D).astype(jnp.bfloat16), layer_w[5], layer_b[5])
            hidden = layer_norm(hidden + cross_out, ln_gain[layer_idx, 1], ln_bias[layer_idx, 1])
            inner_act = jax.nn.gelu(project(hidden.astype(jnp.bfloat16), fc1_w[layer_idx], fc1_b[layer_idx]), approximate=False).astype(jnp.bfloat16)
            ffn_out = project(inner_act, fc2_w[layer_idx], fc2_b[layer_idx])
            hidden = layer_norm(hidden + ffn_out, ln_gain[layer_idx, 2], ln_bias[layer_idx, 2])
        step_logits.append(jnp.dot(hidden.astype(jnp.bfloat16), tok_embed.T, preferred_element_type=jnp.float32) + logit_bias)
    return jnp.stack(step_logits), jnp.stack(cache_k), jnp.stack(cache_v)
```

```python
import functools

import jax
import jax.numpy as jnp
from jax import lax
from jax.experimental import pallas as pl
from jax.experimental.pallas import tpu as pltpu
from jax.sharding import PartitionSpec as P

LN_EPS = 1e-5


MESH = pl.DeviceIdType.MESH
ORDER_E, ORDER_A, ORDER_B = 'xyz', 'zxy', 'zyx'
NUM_Z = 4
OFFSETS = [(dz, fx, fy) for dz in range(1 - NUM_Z, NUM_Z) for fx in (0, 1) for fy in (0, 1)]


class Grid:
    def __init__(self):
        self.me = lax.axis_index('fsdp')
        self.z = self.me // 8
        self.step_x = 2 - 4 * ((self.me // 2) % 2)
        self.step_y = 4 - 8 * ((self.me // 4) % 2)
        self.step_core = 1 - 2 * (self.me % 2)

    def source(self, offset):
        dz, fx, fy = offset
        return self.me + 8 * dz + fx * self.step_x + fy * self.step_y

    def exists(self, dz):
        if dz > 0:
            return self.z < NUM_Z - dz
        return self.z >= -dz

    def barrier(self):
        sem = pltpu.get_barrier_semaphore()
        for step in (self.step_x, self.step_y, self.step_core):
            pl.semaphore_signal(sem, inc=1, device_id=(self.me + step,), device_id_type=MESH)
        for dz in (1, -1):
            @pl.when(self.exists(dz))
            def _():
                pl.semaphore_signal(sem, inc=1, device_id=(self.me + 8 * dz,), device_id_type=MESH)
        inner = jnp.logical_and(self.z > 0, self.z < NUM_Z - 1)

        @pl.when(inner)
        def _():
            pl.semaphore_wait(sem, 5)

        @pl.when(jnp.logical_not(inner))
        def _():
            pl.semaphore_wait(sem, 4)


def onward(offset, order):
    dz, fx, fy = offset
    parts = {'x': fx, 'y': fy, 'z': dz}
    last = max([place for place, dim in enumerate(order) if parts[dim]], default=-1)
    sends = [('c', 0)]
    if last >= 0 and order[last] == 'z':
        sends.append(('u', 1) if dz < 0 else ('d', -1))
    for dim in order[last + 1:]:
        sends += [('u', 1), ('d', -1)] if dim == 'z' else [(dim, 0)]
    return sends


def hops(offset):
    return abs(offset[0]) + offset[1] + offset[2]


WAYS = 'xyudc'


class Gather:
    def __init__(self, grid, pieces, send_sem, recv_sem):
        self.grid, self.pieces, self.send_sem, self.recv_sem = grid, pieces, send_sem, recv_sem

    def copy(self, number, offset, way):
        grid = self.grid
        source = grid.source(offset)
        own, place, _ = self.pieces[number]
        step = {'x': grid.step_x, 'y': grid.step_y, 'u': 8, 'd': -8, 'c': grid.step_core}[way]
        here = place(source)
        return pltpu.make_async_remote_copy(
            src_ref=own if hops(offset) == 0 else here, dst_ref=here,
            send_sem=self.send_sem.at[number, source // 2, WAYS.index(way)], recv_sem=self.recv_sem.at[number, source],
            device_id=(grid.me + step,), device_id_type=MESH)

    def each_send(self, number, offset, act):
        for way, dz in onward(offset, self.pieces[number][2]):
            if dz:
                @pl.when(self.grid.exists(dz))
                def _(way=way):
                    act(self.copy(number, offset, way))
            else:
                act(self.copy(number, offset, way))

    def forward(self, number, count):
        for offset in OFFSETS:
            if hops(offset) != count:
                continue

            def pass_on(offset=offset):
                if count:
                    self.wait(number, self.grid.source(offset))
                self.each_send(number, offset, lambda copy: copy.start())

            if offset[0]:
                pl.when(self.grid.exists(offset[0]))(pass_on)
            else:
                pass_on()

    def wait(self, number, source):
        place = self.pieces[number][1](source)
        pltpu.make_async_remote_copy(
            src_ref=place, dst_ref=place, send_sem=self.recv_sem.at[number, source], recv_sem=self.recv_sem.at[number, source],
            device_id=(self.grid.me,), device_id_type=MESH).wait_recv()

    def finish(self, number):
        other = self.grid.step_core
        for offset in OFFSETS:
            def drain(offset=offset):
                self.wait(number, self.grid.source(offset) + other)
                self.each_send(number, offset, lambda copy: copy.wait_send())

            if offset[0]:
                pl.when(self.grid.exists(offset[0]))(drain)
            else:
                drain()


MAX_HOPS = NUM_Z + 1
WEIGHT_GROUPS = ((0, 3, ORDER_E), (3, 5, ORDER_A), (8, 6, ORDER_B))


def weights_kernel(in_ref, out_ref, send_sem, recv_sem, own_sem):
    grid = Grid()
    num_layers, num_blocks, share, _ = in_ref.shape

    def piece(layer, first, count, order):
        return (in_ref.at[layer, pl.ds(first, count)],
                lambda source: out_ref.at[layer, pl.ds(first, count), pl.ds(pl.multiple_of(share * source, share), share), :], order)

    pieces = [piece(layer, *group) for layer in range(num_layers) for group in WEIGHT_GROUPS]
    gather = Gather(grid, pieces, send_sem, recv_sem)
    own = pltpu.make_async_copy(in_ref, out_ref.at[:, :, pl.ds(pl.multiple_of(share * grid.me, share), share), :], own_sem)
    own.start()
    grid.barrier()
    per_layer = len(WEIGHT_GROUPS)
    for count in range(MAX_HOPS + 2):
        for number in range(len(pieces)):
            hop = count - number // per_layer
            if 0 <= hop <= MAX_HOPS:
                gather.forward(number, hop)
    for number in range(len(pieces)):
        gather.finish(number)
    own.wait()


def gather_weights(packed):
    num_layers, num_blocks, share, width = packed.shape
    num_pieces = num_layers * len(WEIGHT_GROUPS)
    return pl.pallas_call(
        weights_kernel,
        out_shape=jax.ShapeDtypeStruct((num_layers, num_blocks, share * 32, width), packed.dtype),
        in_specs=[pl.BlockSpec(memory_space=pl.ANY)],
        out_specs=pl.BlockSpec(memory_space=pl.ANY),
        scratch_shapes=[pltpu.SemaphoreType.DMA((num_pieces, 16, len(WAYS))), pltpu.SemaphoreType.DMA((num_pieces, 32)), pltpu.SemaphoreType.DMA],
        compiler_params=pltpu.CompilerParams(collective_id=1, has_side_effects=True),
        cost_estimate=pl.CostEstimate(flops=200_000_000_000, bytes_accessed=120_000_000, transcendentals=0),
        name='gather_weights',
    )(packed)


def layer_norm(values, gain_row, shift_row):
    row_mean = values.mean(-1, keepdims=True)
    centered = values - row_mean
    variance = (centered * centered).mean(-1, keepdims=True)
    return centered * lax.rsqrt(variance + LN_EPS) * gain_row.astype(jnp.float32) + shift_row.astype(jnp.float32)


def attend(query_rows, key_rows, val_rows, valid_len):
    scores = jnp.einsum('sbhd,bthd->sbht', query_rows, key_rows, preferred_element_type=jnp.float32)
    valid_mask = jnp.arange(key_rows.shape[1])[None, None, None, :] < valid_len[:, :, None, None]
    scores = jnp.where(valid_mask, scores, -jnp.inf)
    weights = jnp.exp(scores - scores.max(-1, keepdims=True))
    mixed_rows = jnp.einsum('sbht,bthd->sbhd', weights.astype(jnp.bfloat16), val_rows, preferred_element_type=jnp.float32)
    return mixed_rows / weights.sum(-1)[:, :, :, None]


def project(act_rows, weight, bias_row):
    return jnp.einsum('...d,de->...e', act_rows, weight, preferred_element_type=jnp.float32) + bias_row


def decoder_layer(hidden, positions, src_len, cache_k, cache_v, cross_k, cross_v, layer_w, layer_b, up_w, up_b, down_w, down_b, ln_gains, ln_shifts):
    num_rows, num_times, num_heads, head_dim = cache_k.shape
    num_steps = hidden.shape[0]
    attn_scale = head_dim ** -0.5
    head_shape = (num_steps, num_rows, num_heads, head_dim)
    act_rows = hidden.astype(jnp.bfloat16)
    self_query = (project(act_rows, layer_w[0], layer_b[0]) * attn_scale).astype(jnp.bfloat16).reshape(head_shape)
    new_key = project(act_rows, layer_w[1], layer_b[1]).astype(jnp.bfloat16).reshape(head_shape)
    new_val = project(act_rows, layer_w[2], layer_b[2]).astype(jnp.bfloat16).reshape(head_shape)
    times = jnp.arange(num_times)[None, :]
    for step in range(num_steps):
        write_mask = (times == positions[:, None] + step)[:, :, None, None]
        cache_k = jnp.where(write_mask, new_key[step][:, None], cache_k)
        cache_v = jnp.where(write_mask, new_val[step][:, None], cache_v)
    steps = jnp.arange(num_steps)[:, None]
    mixed_rows = attend(self_query, cache_k, cache_v, positions[None, :] + steps + 1)
    attn_out = project(mixed_rows.reshape(hidden.shape).astype(jnp.bfloat16), layer_w[3], layer_b[3])
    hidden = layer_norm(hidden + attn_out, ln_gains[0], ln_shifts[0])
    cross_query = (project(hidden.astype(jnp.bfloat16), layer_w[4], layer_b[4]) * attn_scale).astype(jnp.bfloat16).reshape(head_shape)
    mixed_rows = attend(cross_query, cross_k, cross_v, jnp.broadcast_to(src_len[None], (num_steps, num_rows)))
    cross_out = project(mixed_rows.reshape(hidden.shape).astype(jnp.bfloat16), layer_w[5], layer_b[5])
    hidden = layer_norm(hidden + cross_out, ln_gains[1], ln_shifts[1])
    inner = jnp.einsum('sbd,ide->sbie', hidden.astype(jnp.bfloat16), up_w, preferred_element_type=jnp.float32) + up_b.reshape(4, -1)
    inner_act = jax.nn.gelu(inner, approximate=False).astype(jnp.bfloat16)
    ffn_out = jnp.einsum('sbie,ied->sbd', inner_act, down_w, preferred_element_type=jnp.float32) + down_b
    hidden = layer_norm(hidden + ffn_out, ln_gains[2], ln_shifts[2])
    return hidden, cache_k, cache_v


def solution(mesh):
    cache_spec = P(None, 'fsdp')
    in_specs = (P('fsdp'), P('fsdp'), P('fsdp'), cache_spec, cache_spec, cache_spec, cache_spec,
                P(None, None, 'fsdp'), P(None, None, 'fsdp'), P(None, 'fsdp'), P(None, 'fsdp'),
                P(None, 'fsdp'), P(None, 'fsdp'), P(None, None, 'fsdp'), P(None, None, 'fsdp'),
                P('fsdp'), P(), P(), P('fsdp'))
    out_specs = (P(None, None, 'fsdp'), cache_spec, cache_spec)

    def local_decode(tokens, positions, src_len, self_k, self_v, cross_k, cross_v, attn_w, attn_b, fc1_w, fc1_b, fc2_w, fc2_b, ln_gain, ln_bias, tok_embed, pos_embed, emb_norm, logit_bias):
        shard_idx = lax.axis_index('fsdp')
        num_layers = attn_w.shape[0]
        num_rows, num_steps = tokens.shape
        vocab_local = tok_embed.shape[0]
        small = (tokens.T, attn_b, fc1_b, fc2_b, ln_gain, ln_bias)
        packed = jnp.concatenate([part.astype(jnp.float32).reshape(-1) for part in small])
        gathered = lax.all_gather(packed, 'fsdp', axis=0)
        pieces, start = [], 0
        for part in small:
            block = gathered[:, start:start + part.size].reshape((-1,) + part.shape)
            pieces.append(jnp.moveaxis(block, 0, -2).reshape(part.shape[:-1] + (-1,)))
            start += part.size
        all_tokens = pieces[0].astype(jnp.int32)
        all_attn_b, all_fc1_b, all_fc2_b, all_gain, all_shift = pieces[1:]
        local_ids = all_tokens - shard_idx * vocab_local
        owned_mask = (local_ids >= 0) & (local_ids < vocab_local)
        picked = jnp.take(tok_embed, jnp.clip(local_ids, 0, vocab_local - 1), axis=0)
        picked = jnp.where(owned_mask[:, :, None], picked, jnp.zeros_like(picked))
        tok_rows = lax.psum_scatter(picked, 'fsdp', scatter_dimension=1, tiled=True)
        step_pos = positions[None, :] + jnp.arange(num_steps)[:, None]
        start_rows = tok_rows.astype(jnp.float32) + jnp.take(pos_embed, step_pos + 2, axis=0).astype(jnp.float32)
        hidden = layer_norm(start_rows, emb_norm[0], emb_norm[1])
        num_dev = mesh.shape['fsdp']
        depth = attn_w.shape[2]
        width = attn_w.shape[3]
        up_blocks = fc1_w.reshape(num_layers, depth, num_dev, 4, depth).transpose(0, 3, 1, 2, 4).reshape(num_layers, 4, depth, width)
        down_blocks = fc2_w.reshape(num_layers, 4, depth, width)
        packed_w = jnp.concatenate([attn_w[:, :3], attn_w[:, 4:5], up_blocks, attn_w[:, 3:4], attn_w[:, 5:6], down_blocks], axis=1)
        full_w = gather_weights(packed_w)
        all_fc1_b = all_fc1_b.reshape(num_layers, num_dev, 4, depth).transpose(0, 2, 1, 3).reshape(num_layers, 4 * width)
        cache_k, cache_v = [], []
        for layer_idx in range(num_layers):
            blocks = full_w[layer_idx]
            layer_w = (blocks[0], blocks[1], blocks[2], blocks[8], blocks[3], blocks[9])
            up_w, down_w = blocks[4:8], blocks[10:14]
            hidden, new_k, new_v = decoder_layer(
                hidden, positions, src_len, self_k[layer_idx], self_v[layer_idx], cross_k[layer_idx], cross_v[layer_idx],
                layer_w, all_attn_b[layer_idx], up_w, all_fc1_b[layer_idx], down_w, all_fc2_b[layer_idx], all_gain[layer_idx], all_shift[layer_idx])
            cache_k.append(new_k)
            cache_v.append(new_v)
        all_rows = lax.all_gather(hidden.astype(jnp.bfloat16), 'fsdp', axis=1, tiled=True)
        logits = jnp.einsum('vd,sbd->vsb', tok_embed, all_rows, preferred_element_type=jnp.float32) + logit_bias[:, None, None]
        return jnp.transpose(logits, (1, 2, 0)), jnp.stack(cache_k), jnp.stack(cache_v)

    return jax.shard_map(local_decode, mesh=mesh, in_specs=in_specs, out_specs=out_specs, check_vma=False)
```

```python
import functools

import jax
import jax.numpy as jnp
from jax import lax
from jax.experimental import pallas as pl
from jax.experimental.pallas import tpu as pltpu
from jax.sharding import PartitionSpec as P

LN_EPS = 1e-5


MESH = pl.DeviceIdType.MESH
ORDER_E, ORDER_A, ORDER_B = 'xyz', 'zxy', 'zyx'
NUM_Z = 4
OFFSETS = [(dz, fx, fy) for dz in range(1 - NUM_Z, NUM_Z) for fx in (0, 1) for fy in (0, 1)]


class Grid:
    def __init__(self):
        self.me = lax.axis_index('fsdp')
        self.z = self.me // 8
        self.step_x = 2 - 4 * ((self.me // 2) % 2)
        self.step_y = 4 - 8 * ((self.me // 4) % 2)
        self.step_core = 1 - 2 * (self.me % 2)

    def source(self, offset):
        dz, fx, fy = offset
        return self.me + 8 * dz + fx * self.step_x + fy * self.step_y

    def exists(self, dz):
        if dz > 0:
            return self.z < NUM_Z - dz
        return self.z >= -dz

    def neighbour_barrier(self):
        sem = pltpu.get_barrier_semaphore()
        for step in (self.step_x, self.step_y, self.step_core):
            pl.semaphore_signal(sem, inc=1, device_id=(self.me + step,), device_id_type=MESH)
        for dz in (1, -1):
            @pl.when(self.exists(dz))
            def _():
                pl.semaphore_signal(sem, inc=1, device_id=(self.me + 8 * dz,), device_id_type=MESH)
        inner = jnp.logical_and(self.z > 0, self.z < NUM_Z - 1)

        @pl.when(inner)
        def _():
            pl.semaphore_wait(sem, 5)

        @pl.when(jnp.logical_not(inner))
        def _():
            pl.semaphore_wait(sem, 4)


NUM_DEV = 32


class Exchange:
    def __init__(self, block, place, send_sem, recv_sem):
        self.me = lax.axis_index('fsdp')
        self.block, self.place, self.send_sem, self.recv_sem = block, place, send_sem, recv_sem

    def peer(self, step):
        return lax.rem(self.me + step, NUM_DEV)

    def copy(self, step, source):
        peer = self.peer(step)
        return pltpu.make_async_remote_copy(
            src_ref=self.block(peer), dst_ref=self.place(source), send_sem=self.send_sem.at[step], recv_sem=self.recv_sem.at[source],
            device_id=(peer,), device_id_type=MESH)

    def signal(self):
        barrier = pltpu.get_barrier_semaphore()

        @pl.loop(1, NUM_DEV)
        def _(step):
            pl.semaphore_signal(barrier, inc=1, device_id=(self.peer(step),), device_id_type=MESH)

    def barrier(self):
        pl.semaphore_wait(pltpu.get_barrier_semaphore(), NUM_DEV - 1)

    def start(self):
        @pl.loop(1, NUM_DEV)
        def _(step):
            self.copy(step, self.me).start()

    def wait_recv(self):
        @pl.loop(1, NUM_DEV)
        def _(step):
            self.copy(step, self.peer(step)).wait_recv()

    def wait_send(self):
        @pl.loop(1, NUM_DEV)
        def _(step):
            self.copy(step, self.me).wait_send()


def onward(offset, order):
    dz, fx, fy = offset
    parts = {'x': fx, 'y': fy, 'z': dz}
    last = max([place for place, dim in enumerate(order) if parts[dim]], default=-1)
    sends = [('c', 0)]
    if last >= 0 and order[last] == 'z':
        sends.append(('u', 1) if dz < 0 else ('d', -1))
    for dim in order[last + 1:]:
        sends += [('u', 1), ('d', -1)] if dim == 'z' else [(dim, 0)]
    return sends


def hops(offset):
    return abs(offset[0]) + offset[1] + offset[2]


WAYS = 'xyudc'


MAX_HOPS = NUM_Z + 1


class Gather:
    def __init__(self, grid, pieces, waves, send_sem, recv_sem):
        self.grid, self.pieces, self.waves, self.send_sem, self.recv_sem = grid, pieces, waves, send_sem, recv_sem

    def copy(self, wave, number, piece, offset, way):
        grid = self.grid
        source = grid.source(offset)
        own, place, _ = piece
        step = {'x': grid.step_x, 'y': grid.step_y, 'u': 8, 'd': -8, 'c': grid.step_core}[way]
        here = place(source)
        return pltpu.make_async_remote_copy(
            src_ref=own if hops(offset) == 0 else here, dst_ref=here,
            send_sem=self.send_sem.at[wave, number, source // 2, WAYS.index(way)], recv_sem=self.recv_sem.at[wave, number, source],
            device_id=(grid.me + step,), device_id_type=MESH)

    def each_send(self, wave, number, piece, offset, act):
        for way, dz in onward(offset, piece[2]):
            if dz:
                @pl.when(self.grid.exists(dz))
                def _(way=way):
                    act(self.copy(wave, number, piece, offset, way))
            else:
                act(self.copy(wave, number, piece, offset, way))

    def wait(self, wave, number, piece, source):
        place = piece[1](source)
        pltpu.make_async_remote_copy(
            src_ref=place, dst_ref=place, send_sem=self.recv_sem.at[wave, number, source], recv_sem=self.recv_sem.at[wave, number, source],
            device_id=(self.grid.me,), device_id_type=MESH).wait_recv()

    def each_offset(self, count, act):
        for offset in OFFSETS:
            if count is None or hops(offset) == count:
                if offset[0]:
                    pl.when(self.grid.exists(offset[0]))(functools.partial(act, offset))
                else:
                    act(offset)

    def forward(self, wave, count):
        for number, piece in enumerate(self.pieces(wave)):
            def pass_on(offset, number=number, piece=piece):
                if count:
                    self.wait(wave, number, piece, self.grid.source(offset))
                self.each_send(wave, number, piece, offset, lambda copy: copy.start())

            self.each_offset(count, pass_on)

    def run(self, first=True):
        if first:
            self.forward(0, 0)

        def cross(wave, carry):
            for count in range(1, MAX_HOPS + 1):
                if count == 3 and self.waves > 1:
                    @pl.when(wave + 1 < self.waves)
                    def _():
                        self.forward(wave + 1, 0)
                self.forward(wave, count)
            return carry

        def finish(wave, carry):
            for number, piece in enumerate(self.pieces(wave)):
                def drain(offset, number=number, piece=piece):
                    self.wait(wave, number, piece, self.grid.source(offset) + self.grid.step_core)
                    self.each_send(wave, number, piece, offset, lambda copy: copy.wait_send())

                self.each_offset(None, drain)
            return carry

        lax.fori_loop(0, self.waves, cross, 0)
        lax.fori_loop(0, self.waves, finish, 0)


def rows_at(ref, lead, share):
    return lambda source: ref.at[(*lead, pl.ds(pl.multiple_of(share * source, share), share))]


ROW_FC2, ROW_GAIN, ROW_SHIFT, ROW_TOKEN, ROW_FC1 = 12, 14, 20, 26, 28
SLOTS = 16


def weights_kernel(small, tail, embed_hbm, attn_ref, fc1_ref, fc2_ref, table_out, rows_out, attn_out, fc1_out, fc2_out,
                   ids, ranks, onehot, picks, embed, send_sem, recv_sem, own_sem, small_send, small_recv, row_send, row_recv):
    grid = Grid()
    me = grid.me
    num_layers = attn_ref.shape[0]
    share = small.shape[1]
    table = Exchange(lambda peer: small, lambda source: table_out.at[source], small_send, small_recv)
    rows = Exchange(lambda peer: picks.at[peer], lambda source: rows_out.at[source], row_send, row_recv)
    table.signal()

    def pieces(layer):
        blocks = [(attn_ref.at[layer, pl.ds(first, count)], rows_at(attn_out, (layer, pl.ds(first, count)), attn_ref.shape[2]), order)
                  for first, count, order in ((0, 3, ORDER_E), (5, 1, ORDER_A), (3, 2, ORDER_B))]
        return blocks + [(fc1_ref.at[layer], rows_at(fc1_out, (layer,), fc1_ref.shape[1]), ORDER_A),
                         (fc2_ref.at[layer], rows_at(fc2_out, (layer,), fc2_ref.shape[1]), ORDER_B)]

    own = [
        pltpu.make_async_copy(attn_ref, rows_at(attn_out, (slice(None), slice(None)), attn_ref.shape[2])(me), own_sem.at[0]),
        pltpu.make_async_copy(fc1_ref, rows_at(fc1_out, (slice(None),), fc1_ref.shape[1])(me), own_sem.at[1]),
        pltpu.make_async_copy(fc2_ref, rows_at(fc2_out, (slice(None),), fc2_ref.shape[1])(me), own_sem.at[2]),
    ]
    for copy in own:
        copy.start()
    vocab = embed_hbm.shape[0]
    body = embed.shape[0] - tail.shape[0]
    embed_copy = pltpu.make_async_copy(embed_hbm.at[pl.ds(0, body)], embed.at[pl.ds(0, body)], own_sem.at[3])
    embed_copy.start()
    embed[pl.ds(body, tail.shape[0])] = tail[...]
    table_out[me] = small[...]
    table.barrier()
    table.start()
    gather = Gather(grid, pieces, num_layers, send_sem, recv_sem)
    gather.forward(0, 0)

    table.wait_recv()
    wanted = jnp.concatenate([table_out[:, ROW_TOKEN + step, :] for step in range(ids.shape[1] // share)], axis=1) - (me * vocab).astype(jnp.float32)
    mine = jnp.logical_and(wanted >= 0, wanted < vocab)
    number = ids.shape[1]
    before = lax.broadcasted_iota(jnp.int32, (number, number), 0) <= lax.broadcasted_iota(jnp.int32, (number, number), 1)
    rank = jnp.dot(jnp.where(mine, 1.0, 0.0).astype(jnp.bfloat16), jnp.where(before, 1.0, 0.0).astype(jnp.bfloat16), preferred_element_type=jnp.float32)
    ids[pl.ds(0, NUM_DEV)] = wanted
    ranks[pl.ds(0, NUM_DEV)] = jnp.where(mine, rank, 0.0)
    slot = lax.broadcasted_iota(jnp.int32, (SLOTS, number), 0).astype(jnp.float32) + 1.0
    line = lax.broadcasted_iota(jnp.int32, (SLOTS, embed.shape[0]), 1).astype(jnp.float32)

    @pl.loop(0, NUM_DEV)
    def _(peer):
        hit = ranks[pl.ds(peer, 1), :] == slot
        chosen = jnp.sum(jnp.where(hit, ids[pl.ds(peer, 1), :] + 1.0, 0.0), axis=1, keepdims=True)
        onehot[pl.ds(pl.multiple_of(peer * SLOTS, SLOTS), SLOTS), :] = jnp.where(line == chosen - 1.0, 1.0, 0.0).astype(jnp.bfloat16)

    group = 128 // SLOTS
    embed_copy.wait()

    @pl.loop(0, NUM_DEV // group)
    def _(part):
        found = jnp.dot(onehot[pl.ds(pl.multiple_of(part * 128, 128), 128), :], embed[...], preferred_element_type=jnp.float32)
        picks[pl.ds(part * group, group)] = found.astype(jnp.bfloat16).reshape(group, SLOTS, found.shape[1])

    rows_out[me] = picks[me]
    rows.start()
    gather.run(first=False)
    rows.wait_recv()
    rows.wait_send()
    table.wait_send()
    for copy in own:
        copy.wait()


def gather_weights(small, num_tokens, embed, attn_w, fc1_w, fc2_w):
    lanes = 128
    body = embed.shape[0] // lanes * lanes
    tail = jnp.zeros((lanes, embed.shape[1]), embed.dtype).at[:embed.shape[0] - body].set(embed[body:])
    def whole(array, dim):
        return jax.ShapeDtypeStruct(array.shape[:dim] + (array.shape[dim] * NUM_DEV,) + array.shape[dim + 1:], array.dtype)

    any_spec = pl.BlockSpec(memory_space=pl.ANY)
    vmem = pl.BlockSpec(memory_space=pltpu.VMEM)
    num_layers = attn_w.shape[0]
    width = embed.shape[1]
    dma = pltpu.SemaphoreType.DMA
    return pl.pallas_call(
        weights_kernel,
        out_shape=(jax.ShapeDtypeStruct((NUM_DEV,) + small.shape, jnp.float32), jax.ShapeDtypeStruct((NUM_DEV, SLOTS, width), embed.dtype),
                   whole(attn_w, 2), whole(fc1_w, 1), whole(fc2_w, 1)),
        in_specs=[vmem] * 2 + [any_spec] * 4,
        out_specs=(vmem, vmem) + (any_spec,) * 3,
        scratch_shapes=[
            pltpu.VMEM((NUM_DEV + 8, num_tokens), jnp.float32), pltpu.VMEM((NUM_DEV + 8, num_tokens), jnp.float32),
            pltpu.VMEM((NUM_DEV * SLOTS, body + lanes), jnp.bfloat16), pltpu.VMEM((NUM_DEV, SLOTS, width), jnp.bfloat16), pltpu.VMEM((body + lanes, width), jnp.bfloat16),
            dma((num_layers, 5, 16, len(WAYS))), dma((num_layers, 5, NUM_DEV)), dma((4,)),
            dma((NUM_DEV,)), dma((NUM_DEV,)), dma((NUM_DEV,)), dma((NUM_DEV,)),
        ],
        compiler_params=pltpu.CompilerParams(collective_id=1, has_side_effects=True, vmem_limit_bytes=40 * 1024 * 1024),
        cost_estimate=pl.CostEstimate(flops=200_000_000_000, bytes_accessed=120_000_000, transcendentals=0),
        name='gather_weights',
    )(small, tail, embed, attn_w, fc1_w, fc2_w)


def rows_kernel(in_ref, out_ref, send_sem, recv_sem, own_sem):
    grid = Grid()
    share = in_ref.shape[1]
    half = share // 2

    def piece(step, part, order):
        return (in_ref.at[step, pl.ds(part * half, half)],
                lambda source: out_ref.at[step, pl.ds(pl.multiple_of(share * source + part * half, half), half)], order)

    own = pltpu.make_async_copy(in_ref, out_ref.at[:, pl.ds(pl.multiple_of(share * grid.me, share), share)], own_sem)
    own.start()
    grid.neighbour_barrier()
    Gather(grid, lambda wave: [piece(0, 0, 'xzy'), piece(0, 1, 'yzx'), piece(1, 0, ORDER_A), piece(1, 1, ORDER_B)], 1, send_sem, recv_sem).run()
    own.wait()


def gather_rows(rows):
    steps, share, width = rows.shape
    vmem = pl.BlockSpec(memory_space=pltpu.VMEM)
    return pl.pallas_call(
        rows_kernel,
        out_shape=jax.ShapeDtypeStruct((steps, share * 32, width), rows.dtype),
        in_specs=[vmem],
        out_specs=vmem,
        scratch_shapes=[pltpu.SemaphoreType.DMA((1, 4, 16, len(WAYS))), pltpu.SemaphoreType.DMA((1, 4, 32)), pltpu.SemaphoreType.DMA],
        compiler_params=pltpu.CompilerParams(collective_id=2, has_side_effects=True),
        cost_estimate=pl.CostEstimate(flops=20_000_000_000, bytes_accessed=8_000_000, transcendentals=0),
        name='gather_rows',
    )(rows)


def norm_rows(values, gain_row, shift_row):
    row_mean = jnp.mean(values, axis=-1, keepdims=True)
    centered = values - row_mean
    variance = jnp.mean(centered * centered, axis=-1, keepdims=True)
    return centered * lax.rsqrt(variance + LN_EPS) * gain_row + shift_row


UNROLL = 4


def layers_kernel(pos_ref, len_ref, tok_ref, posrow_ref, embnorm_ref, table_ref, fc1b_ref, attn_hbm, fc1_hbm, fc2_hbm,
                  self_k_hbm, self_v_hbm, cross_k_hbm, cross_v_hbm, rows_ref, out_k_hbm, out_v_hbm,
                  attn_buf, fc1_buf, fc2_buf, kbuf, vbuf, ckbuf, cvbuf, q3, k3, v3, o3, xs, inner, w_sem, c_sem, o_sem):
    num_layers, num_rows, num_times, num_heads, head_dim = kbuf.shape
    num_steps = xs.shape[0] // num_rows
    width = xs.shape[1]
    fat = num_steps * num_heads

    def weight_copy(layer, which):
        if which < 6:
            return pltpu.make_async_copy(attn_hbm.at[layer, which], attn_buf.at[which], w_sem.at[which])
        if which == 6:
            return pltpu.make_async_copy(fc1_hbm.at[layer], fc1_buf, w_sem.at[6])
        return pltpu.make_async_copy(fc2_hbm.at[layer], fc2_buf, w_sem.at[7])

    def self_copy(layer):
        return (pltpu.make_async_copy(self_k_hbm.at[layer], kbuf.at[layer], c_sem.at[0, layer]),
                pltpu.make_async_copy(self_v_hbm.at[layer], vbuf.at[layer], c_sem.at[1, layer]))

    def cross_copy(layer):
        return (pltpu.make_async_copy(cross_k_hbm.at[layer], ckbuf, c_sem.at[2, 0]),
                pltpu.make_async_copy(cross_v_hbm.at[layer], cvbuf, c_sem.at[2, 1]))

    def out_copy(layer):
        return (pltpu.make_async_copy(kbuf.at[layer], out_k_hbm.at[layer], o_sem.at[0, layer]),
                pltpu.make_async_copy(vbuf.at[layer], out_v_hbm.at[layer], o_sem.at[1, layer]))

    for which in (0, 1, 2):
        weight_copy(0, which).start()
    for copy in self_copy(0):
        copy.start()
    for which in (3, 4):
        weight_copy(0, which).start()
    for copy in cross_copy(0):
        copy.start()
    for which in (5, 6, 7):
        weight_copy(0, which).start()
    for layer in range(1, num_layers):
        for copy in self_copy(layer):
            copy.start()

    gain = embnorm_ref[pl.ds(0, 1), :].astype(jnp.float32)
    shift = embnorm_ref[pl.ds(1, 1), :].astype(jnp.float32)
    xs[...] = norm_rows(tok_ref[...].astype(jnp.float32) + posrow_ref[...].astype(jnp.float32), gain, shift)

    row_id = lax.broadcasted_iota(jnp.int32, (fat, num_times * num_heads), 0)
    col_id = lax.broadcasted_iota(jnp.int32, (fat, num_times * num_heads), 1)
    same_head = lax.rem(row_id, num_heads) == lax.rem(col_id, num_heads)
    step_id, time_id = row_id // num_heads, col_id // num_heads
    self_rank = jnp.where(same_head, time_id - step_id, num_times * 2)
    cross_rank = jnp.where(same_head, time_id, num_times * 2)

    def row(index):
        return table_ref[pl.ds(index, 1), :]

    def project(values, which, layer):
        out = jnp.dot(values, attn_buf[which], preferred_element_type=jnp.float32) + row(layer * 6 + which)
        return out

    def refill(layer, which):
        @pl.when(layer + 1 < num_layers)
        def _():
            weight_copy(layer + 1, which).start()

    def split_heads(values, ref):
        for head in range(num_heads):
            ref[:, head, :] = values[:, head * head_dim:(head + 1) * head_dim]

    def join_heads(ref):
        return jnp.concatenate([ref[:, head, :] for head in range(num_heads)], axis=1)

    def per_step(ref, index):
        return jnp.concatenate([ref[step * num_rows + index] for step in range(num_steps)], axis=0)

    def attend_one(index, keys, vals, rank, last):
        query = per_step(q3, index).astype(jnp.bfloat16)
        keys = keys.reshape(num_times * num_heads, head_dim)
        vals = vals.reshape(num_times * num_heads, head_dim)
        scores = lax.dot_general(query, keys, (((1,), (1,)), ((), ())), preferred_element_type=jnp.float32)
        scores = jnp.where(rank <= last, scores, -jnp.inf)
        weights = jnp.exp(scores - jnp.max(scores, axis=-1, keepdims=True))
        total = jnp.sum(weights, axis=-1, keepdims=True)
        mixed = jnp.dot(weights.astype(jnp.bfloat16), vals, preferred_element_type=jnp.float32) / total
        for step in range(num_steps):
            o3[step * num_rows + index] = mixed[step * num_heads:(step + 1) * num_heads]

    def layer_body(layer, carry):
        scale = head_dim ** -0.5
        act = xs[...].astype(jnp.bfloat16)
        for which, ref in ((0, q3), (1, k3), (2, v3)):
            weight_copy(layer, which).wait()
            out = project(act, which, layer)
            split_heads(out * scale if which == 0 else out, ref)
            refill(layer, which)
        for copy in self_copy(layer):
            copy.wait()

        def self_group(group, carry):
            for lane in range(UNROLL):
                index = group * UNROLL + lane
                pos = pos_ref[index]
                for step in range(num_steps):
                    kbuf[layer, index, pos + step] = k3[step * num_rows + index].astype(jnp.bfloat16)
                    vbuf[layer, index, pos + step] = v3[step * num_rows + index].astype(jnp.bfloat16)
                attend_one(index, kbuf[layer, index], vbuf[layer, index], self_rank, pos)
            return carry

        lax.fori_loop(0, num_rows // UNROLL, self_group, 0)
        for copy in out_copy(layer):
            copy.start()
        weight_copy(layer, 3).wait()
        mixed = join_heads(o3).astype(jnp.bfloat16)
        out = project(mixed, 3, layer)
        refill(layer, 3)
        xs[...] = norm_rows(xs[...] + out, row(ROW_GAIN + layer * 3), row(ROW_SHIFT + layer * 3))

        weight_copy(layer, 4).wait()
        split_heads(project(xs[...].astype(jnp.bfloat16), 4, layer) * scale, q3)
        refill(layer, 4)
        for copy in cross_copy(layer):
            copy.wait()

        def cross_group(group, carry):
            for lane in range(UNROLL):
                index = group * UNROLL + lane
                attend_one(index, ckbuf[index], cvbuf[index], cross_rank, len_ref[index] - 1)
            return carry

        lax.fori_loop(0, num_rows // UNROLL, cross_group, 0)

        @pl.when(layer + 1 < num_layers)
        def _():
            for copy in cross_copy(layer + 1):
                copy.start()

        weight_copy(layer, 5).wait()
        mixed = join_heads(o3).astype(jnp.bfloat16)
        out = project(mixed, 5, layer)
        refill(layer, 5)
        xs[...] = norm_rows(xs[...] + out, row(ROW_GAIN + layer * 3 + 1), row(ROW_SHIFT + layer * 3 + 1))

        weight_copy(layer, 6).wait()
        act = xs[...].astype(jnp.bfloat16)
        tile = 512

        def up_tile(index, carry):
            cols = pl.ds(pl.multiple_of(index * tile, tile), tile)
            out = jnp.dot(act, fc1_buf[:, cols], preferred_element_type=jnp.float32) + fc1b_ref[pl.ds(layer, 1), cols]
            inner[:, cols] = (0.5 * out * (1.0 + lax.erf(out * (2.0 ** -0.5)))).astype(jnp.bfloat16)
            return carry

        lax.fori_loop(0, fc1_buf.shape[1] // tile, up_tile, 0)
        refill(layer, 6)
        weight_copy(layer, 7).wait()

        def down_tile(index, total):
            cols = pl.ds(pl.multiple_of(index * tile, tile), tile)
            return total + jnp.dot(inner[:, cols], fc2_buf[cols, :], preferred_element_type=jnp.float32)

        out = lax.fori_loop(0, fc2_buf.shape[0] // tile, down_tile, jnp.zeros(xs.shape, jnp.float32)) + row(ROW_FC2 + layer)
        refill(layer, 7)
        xs[...] = norm_rows(xs[...] + out, row(ROW_GAIN + layer * 3 + 2), row(ROW_SHIFT + layer * 3 + 2))
        return carry

    lax.fori_loop(0, num_layers, layer_body, 0)
    rows_ref[...] = xs[...].astype(jnp.bfloat16)
    for layer in range(num_layers):
        for copy in out_copy(layer):
            copy.wait()


def run_layers(positions, src_len, tok_rows, pos_rows, emb_norm, table, fc1_b, attn_full, fc1_full, fc2_full, self_k, self_v, cross_k, cross_v):
    smem = pl.BlockSpec(memory_space=pltpu.SMEM)
    vmem = pl.BlockSpec(memory_space=pltpu.VMEM)
    any_spec = pl.BlockSpec(memory_space=pl.ANY)
    num_tok, width = tok_rows.shape
    heads, dim = self_k.shape[3:]
    bf16, f32 = jnp.bfloat16, jnp.float32
    return pl.pallas_call(
        layers_kernel,
        out_shape=(jax.ShapeDtypeStruct((num_tok, width), bf16), jax.ShapeDtypeStruct(self_k.shape, bf16), jax.ShapeDtypeStruct(self_v.shape, bf16)),
        in_specs=[smem, smem] + [vmem] * 5 + [any_spec] * 7,
        out_specs=(vmem, any_spec, any_spec),
        scratch_shapes=[
            pltpu.VMEM(attn_full.shape[1:], bf16), pltpu.VMEM(fc1_full.shape[1:], bf16), pltpu.VMEM(fc2_full.shape[1:], bf16),
            pltpu.VMEM(self_k.shape, bf16), pltpu.VMEM(self_v.shape, bf16), pltpu.VMEM(cross_k.shape[1:], bf16), pltpu.VMEM(cross_v.shape[1:], bf16),
            pltpu.VMEM((num_tok, heads, dim), f32), pltpu.VMEM((num_tok, heads, dim), f32), pltpu.VMEM((num_tok, heads, dim), f32), pltpu.VMEM((num_tok, heads, dim), f32),
            pltpu.VMEM((num_tok, width), f32), pltpu.VMEM((num_tok, fc1_full.shape[2]), bf16),
            pltpu.SemaphoreType.DMA((8,)), pltpu.SemaphoreType.DMA((3, 2)), pltpu.SemaphoreType.DMA((2, 2)),
        ],
        compiler_params=pltpu.CompilerParams(vmem_limit_bytes=63 * 1024 * 1024),
        cost_estimate=pl.CostEstimate(flops=8_000_000_000, bytes_accessed=110_000_000, transcendentals=4_000_000),
        name='run_layers',
    )(positions, src_len, tok_rows, pos_rows, emb_norm, table, fc1_b, attn_full, fc1_full, fc2_full, self_k, self_v, cross_k, cross_v)


def logits_kernel(emb_ref, rows_ref, bias_ref, out_ref):
    steps, num_rows, _ = rows_ref.shape
    block = emb_ref.shape[0]
    lanes = 128
    stride = steps * num_rows // lanes
    for step in range(steps):
        scores = lax.dot_general(emb_ref[...], rows_ref[step], (((1,), (1,)), ((), ())), preferred_element_type=jnp.float32) + bias_ref[...]
        for part in range(num_rows // lanes):
            out_ref[pl.ds(part * steps + step, block, stride=stride), :] = scores[:, part * lanes:(part + 1) * lanes]


def run_logits(tok_embed, all_rows, bias):
    vocab, width = tok_embed.shape
    steps, num_rows, _ = all_rows.shape
    block = 400
    per = steps * num_rows // 128
    out = pl.pallas_call(
        logits_kernel,
        grid=(pl.cdiv(vocab, block),),
        out_shape=jax.ShapeDtypeStruct((vocab * per, 128), jnp.float32),
        in_specs=[pl.BlockSpec((block, width), lambda i: (i, 0)), pl.BlockSpec((steps, num_rows, width), lambda i: (0, 0, 0)), pl.BlockSpec((block, 1), lambda i: (i, 0))],
        out_specs=pl.BlockSpec((block * per, 128), lambda i: (i, 0)),
        compiler_params=pltpu.CompilerParams(dimension_semantics=('arbitrary',), vmem_limit_bytes=67_043_328),
        cost_estimate=pl.CostEstimate(flops=2 * vocab * width * steps * num_rows, bytes_accessed=20_000_000, transcendentals=0),
        name='run_logits',
    )(tok_embed, all_rows, bias[:, None])
    return out.reshape(vocab, num_rows // 128, steps, 128).transpose(2, 1, 3, 0).reshape(steps, num_rows, vocab)


def solution(mesh):
    cache_spec = P(None, 'fsdp')
    in_specs = (P('fsdp'), P('fsdp'), P('fsdp'), cache_spec, cache_spec, cache_spec, cache_spec,
                P(None, None, 'fsdp'), P(None, None, 'fsdp'), P(None, 'fsdp'), P(None, 'fsdp'),
                P(None, 'fsdp'), P(None, 'fsdp'), P(None, None, 'fsdp'), P(None, None, 'fsdp'),
                P('fsdp'), P(), P(), P('fsdp'))
    out_specs = (P(None, None, 'fsdp'), cache_spec, cache_spec)

    def local_decode(tokens, positions, src_len, self_k, self_v, cross_k, cross_v, attn_w, attn_b, fc1_w, fc1_b, fc2_w, fc2_b, ln_gain, ln_bias, tok_embed, pos_embed, emb_norm, logit_bias):
        shard_idx = lax.axis_index('fsdp')
        num_layers = attn_w.shape[0]
        num_rows, num_steps = tokens.shape
        vocab_local, width = tok_embed.shape
        num_dev = mesh.shape['fsdp']
        small = (attn_b, fc2_b, ln_gain, ln_bias, tokens.T, fc1_b)
        packed = jnp.concatenate([part.astype(jnp.float32).reshape(-1, num_rows) for part in small], axis=0)
        gathered, found, attn_full, fc1_full, fc2_full = gather_weights(packed, num_steps * num_rows, tok_embed, attn_w, fc1_w, fc2_w)
        table = gathered.transpose(1, 0, 2).reshape(packed.shape[0], num_dev * num_rows)
        all_fc1_b = gathered[:, ROW_FC1:].reshape(num_dev, num_layers, -1).transpose(1, 0, 2).reshape(num_layers, -1)
        all_tokens = gathered[:, ROW_TOKEN:ROW_TOKEN + num_steps].astype(jnp.int32).reshape(num_dev, num_steps * num_rows)
        owner = all_tokens // vocab_local
        most = (owner[:, :, None] == jnp.arange(num_dev)).astype(jnp.int32).sum(axis=1).max()
        my_owner = (tokens.T // vocab_local).reshape(-1)
        order = jnp.arange(num_steps * num_rows)
        my_rank = ((my_owner[None, :] == my_owner[:, None]) & (order[None, :] < order[:, None])).astype(jnp.int32).sum(axis=1)

        def few(found):
            line = my_owner * SLOTS + my_rank
            chosen = (line[:, None] == jnp.arange(num_dev * SLOTS)).astype(found.dtype)
            return jnp.dot(chosen, found.reshape(num_dev * SLOTS, width), preferred_element_type=jnp.float32).astype(found.dtype)

        def many(found):
            local = all_tokens - shard_idx * vocab_local
            mine = (local >= 0) & (local < vocab_local)
            rows = jnp.take(tok_embed, jnp.clip(local, 0, vocab_local - 1), axis=0)
            rows = jnp.where(mine[:, :, None], rows, jnp.zeros_like(rows))
            rows = lax.all_to_all(rows, 'fsdp', 0, 0)
            return rows.astype(jnp.float32).sum(axis=0).astype(found.dtype)

        tok_rows = lax.cond(most > SLOTS, many, few, found)
        step_pos = positions[None, :] + jnp.arange(num_steps)[:, None]
        pos_rows = jnp.take(pos_embed, step_pos + 2, axis=0).reshape(num_steps * num_rows, width)
        rows, cache_k, cache_v = run_layers(positions, src_len, tok_rows, pos_rows, emb_norm, table, all_fc1_b, attn_full, fc1_full, fc2_full, self_k, self_v, cross_k, cross_v)
        all_rows = gather_rows(rows.reshape(num_steps, num_rows, width))
        return run_logits(tok_embed, all_rows, logit_bias), cache_k, cache_v

    return jax.shard_map(local_decode, mesh=mesh, in_specs=in_specs, out_specs=out_specs, check_vma=False)
```

```python
import functools

import jax
import jax.numpy as jnp
from jax import lax
from jax.experimental import pallas as pl
from jax.experimental.pallas import tpu as pltpu
from jax.sharding import PartitionSpec as P

LN_EPS = 1e-5


MESH = pl.DeviceIdType.MESH
ORDER_E, ORDER_A, ORDER_B = 'xyz', 'zxy', 'zyx'
NUM_Z = 4
OFFSETS = [(dz, fx, fy) for dz in range(1 - NUM_Z, NUM_Z) for fx in (0, 1) for fy in (0, 1)]


class Grid:
    def __init__(self):
        self.me = lax.axis_index('fsdp')
        self.z = self.me // 8
        self.step_x = 2 - 4 * ((self.me // 2) % 2)
        self.step_y = 4 - 8 * ((self.me // 4) % 2)
        self.step_core = 1 - 2 * (self.me % 2)

    def source(self, offset):
        dz, fx, fy = offset
        return self.me + 8 * dz + fx * self.step_x + fy * self.step_y

    def exists(self, dz):
        if dz > 0:
            return self.z < NUM_Z - dz
        return self.z >= -dz

    def neighbour_barrier(self):
        sem = pltpu.get_barrier_semaphore()
        for step in (self.step_x, self.step_y, self.step_core):
            pl.semaphore_signal(sem, inc=1, device_id=(self.me + step,), device_id_type=MESH)
        for dz in (1, -1):
            @pl.when(self.exists(dz))
            def _():
                pl.semaphore_signal(sem, inc=1, device_id=(self.me + 8 * dz,), device_id_type=MESH)
        inner = jnp.logical_and(self.z > 0, self.z < NUM_Z - 1)

        @pl.when(inner)
        def _():
            pl.semaphore_wait(sem, 5)

        @pl.when(jnp.logical_not(inner))
        def _():
            pl.semaphore_wait(sem, 4)


NUM_DEV = 32


class Exchange:
    def __init__(self, block, place, send_sem, recv_sem):
        self.me = lax.axis_index('fsdp')
        self.block, self.place, self.send_sem, self.recv_sem = block, place, send_sem, recv_sem

    def peer(self, step):
        return lax.rem(self.me + step, NUM_DEV)

    def copy(self, step, source):
        peer = self.peer(step)
        return pltpu.make_async_remote_copy(
            src_ref=self.block(peer), dst_ref=self.place(source), send_sem=self.send_sem.at[step], recv_sem=self.recv_sem.at[source],
            device_id=(peer,), device_id_type=MESH)

    def signal(self):
        barrier = pltpu.get_barrier_semaphore()

        @pl.loop(1, NUM_DEV)
        def _(step):
            pl.semaphore_signal(barrier, inc=1, device_id=(self.peer(step),), device_id_type=MESH)

    def barrier(self):
        pl.semaphore_wait(pltpu.get_barrier_semaphore(), NUM_DEV - 1)

    def start(self):
        @pl.loop(1, NUM_DEV)
        def _(step):
            self.copy(step, self.me).start()

    def wait_recv(self):
        @pl.loop(1, NUM_DEV)
        def _(step):
            self.copy(step, self.peer(step)).wait_recv()

    def wait_send(self):
        @pl.loop(1, NUM_DEV)
        def _(step):
            self.copy(step, self.me).wait_send()


def onward(offset, order):
    dz, fx, fy = offset
    parts = {'x': fx, 'y': fy, 'z': dz}
    last = max([place for place, dim in enumerate(order) if parts[dim]], default=-1)
    sends = [('c', 0)]
    if last >= 0 and order[last] == 'z':
        sends.append(('u', 1) if dz < 0 else ('d', -1))
    for dim in order[last + 1:]:
        sends += [('u', 1), ('d', -1)] if dim == 'z' else [(dim, 0)]
    return sends


def hops(offset):
    return abs(offset[0]) + offset[1] + offset[2]


WAYS = 'xyudc'


MAX_HOPS = NUM_Z + 1


class Gather:
    def __init__(self, grid, pieces, waves, send_sem, recv_sem):
        self.grid, self.pieces, self.waves, self.send_sem, self.recv_sem = grid, pieces, waves, send_sem, recv_sem

    def copy(self, wave, number, piece, offset, way):
        grid = self.grid
        source = grid.source(offset)
        own, place, _ = piece
        step = {'x': grid.step_x, 'y': grid.step_y, 'u': 8, 'd': -8, 'c': grid.step_core}[way]
        here = place(source)
        return pltpu.make_async_remote_copy(
            src_ref=own if hops(offset) == 0 else here, dst_ref=here,
            send_sem=self.send_sem.at[wave, number, source // 2, WAYS.index(way)], recv_sem=self.recv_sem.at[wave, number, source],
            device_id=(grid.me + step,), device_id_type=MESH)

    def each_send(self, wave, number, piece, offset, act):
        for way, dz in onward(offset, piece[2]):
            if dz:
                @pl.when(self.grid.exists(dz))
                def _(way=way):
                    act(self.copy(wave, number, piece, offset, way))
            else:
                act(self.copy(wave, number, piece, offset, way))

    def wait(self, wave, number, piece, source):
        place = piece[1](source)
        pltpu.make_async_remote_copy(
            src_ref=place, dst_ref=place, send_sem=self.recv_sem.at[wave, number, source], recv_sem=self.recv_sem.at[wave, number, source],
            device_id=(self.grid.me,), device_id_type=MESH).wait_recv()

    def each_offset(self, count, act):
        for offset in OFFSETS:
            if count is None or hops(offset) == count:
                if offset[0]:
                    pl.when(self.grid.exists(offset[0]))(functools.partial(act, offset))
                else:
                    act(offset)

    def forward(self, wave, count):
        for number, piece in enumerate(self.pieces(wave)):
            def pass_on(offset, number=number, piece=piece):
                if count:
                    self.wait(wave, number, piece, self.grid.source(offset))
                self.each_send(wave, number, piece, offset, lambda copy: copy.start())

            self.each_offset(count, pass_on)

    def run(self, first=True):
        if first:
            self.forward(0, 0)

        def cross(wave, carry):
            for count in range(1, MAX_HOPS + 1):
                if count == 3 and self.waves > 1:
                    @pl.when(wave + 1 < self.waves)
                    def _():
                        self.forward(wave + 1, 0)
                self.forward(wave, count)
            return carry

        def finish(wave, carry):
            for number, piece in enumerate(self.pieces(wave)):
                def drain(offset, number=number, piece=piece):
                    self.wait(wave, number, piece, self.grid.source(offset) + self.grid.step_core)
                    self.each_send(wave, number, piece, offset, lambda copy: copy.wait_send())

                self.each_offset(None, drain)
            return carry

        lax.fori_loop(0, self.waves, cross, 0)
        lax.fori_loop(0, self.waves, finish, 0)


def rows_at(ref, lead, share):
    return lambda source: ref.at[(*lead, pl.ds(pl.multiple_of(share * source, share), share))]


ROW_FC2, ROW_GAIN, ROW_SHIFT, ROW_TOKEN, ROW_FC1 = 12, 14, 20, 26, 28
SLOTS = 16


def weights_kernel(small, tail, embed_hbm, attn_ref, fc1_ref, fc2_ref, table_out, rows_out, attn_out, fc1_out, fc2_out,
                   ids, ranks, onehot, picks, embed, send_sem, recv_sem, own_sem, small_send, small_recv, row_send, row_recv):
    grid = Grid()
    me = grid.me
    num_layers = attn_ref.shape[0]
    share = small.shape[1]
    table = Exchange(lambda peer: small, lambda source: table_out.at[source], small_send, small_recv)
    rows = Exchange(lambda peer: picks.at[peer], lambda source: rows_out.at[source], row_send, row_recv)
    table.signal()

    def pieces(layer):
        blocks = [(attn_ref.at[layer, pl.ds(first, count)], rows_at(attn_out, (layer, pl.ds(first, count)), attn_ref.shape[2]), order)
                  for first, count, order in ((0, 3, ORDER_E), (5, 1, ORDER_A), (3, 2, ORDER_B))]
        return blocks + [(fc1_ref.at[layer], rows_at(fc1_out, (layer,), fc1_ref.shape[1]), ORDER_A),
                         (fc2_ref.at[layer], rows_at(fc2_out, (layer,), fc2_ref.shape[1]), ORDER_B)]

    own = [
        pltpu.make_async_copy(attn_ref, rows_at(attn_out, (slice(None), slice(None)), attn_ref.shape[2])(me), own_sem.at[0]),
        pltpu.make_async_copy(fc1_ref, rows_at(fc1_out, (slice(None),), fc1_ref.shape[1])(me), own_sem.at[1]),
        pltpu.make_async_copy(fc2_ref, rows_at(fc2_out, (slice(None),), fc2_ref.shape[1])(me), own_sem.at[2]),
    ]
    for copy in own:
        copy.start()
    vocab = embed_hbm.shape[0]
    body = embed.shape[0] - tail.shape[0]
    embed_copy = pltpu.make_async_copy(embed_hbm.at[pl.ds(0, body)], embed.at[pl.ds(0, body)], own_sem.at[3])
    embed_copy.start()
    embed[pl.ds(body, tail.shape[0])] = tail[...]
    table_out[me] = small[...]
    table.barrier()
    table.start()
    gather = Gather(grid, pieces, num_layers, send_sem, recv_sem)
    gather.forward(0, 0)

    table.wait_recv()
    wanted = jnp.concatenate([table_out[:, ROW_TOKEN + step, :] for step in range(ids.shape[1] // share)], axis=1) - (me * vocab).astype(jnp.float32)
    mine = jnp.logical_and(wanted >= 0, wanted < vocab)
    number = ids.shape[1]
    before = lax.broadcasted_iota(jnp.int32, (number, number), 0) <= lax.broadcasted_iota(jnp.int32, (number, number), 1)
    rank = jnp.dot(jnp.where(mine, 1.0, 0.0).astype(jnp.bfloat16), jnp.where(before, 1.0, 0.0).astype(jnp.bfloat16), preferred_element_type=jnp.float32)
    ids[pl.ds(0, NUM_DEV)] = wanted
    ranks[pl.ds(0, NUM_DEV)] = jnp.where(mine, rank, 0.0)
    slot = lax.broadcasted_iota(jnp.int32, (SLOTS, number), 0).astype(jnp.float32) + 1.0
    line = lax.broadcasted_iota(jnp.int32, (SLOTS, embed.shape[0]), 1).astype(jnp.float32)

    @pl.loop(0, NUM_DEV)
    def _(peer):
        hit = ranks[pl.ds(peer, 1), :] == slot
        chosen = jnp.sum(jnp.where(hit, ids[pl.ds(peer, 1), :] + 1.0, 0.0), axis=1, keepdims=True)
        onehot[pl.ds(pl.multiple_of(peer * SLOTS, SLOTS), SLOTS), :] = jnp.where(line == chosen - 1.0, 1.0, 0.0).astype(jnp.bfloat16)

    group = 128 // SLOTS
    embed_copy.wait()

    @pl.loop(0, NUM_DEV // group)
    def _(part):
        found = jnp.dot(onehot[pl.ds(pl.multiple_of(part * 128, 128), 128), :], embed[...], preferred_element_type=jnp.float32)
        picks[pl.ds(part * group, group)] = found.astype(jnp.bfloat16).reshape(group, SLOTS, found.shape[1])

    rows_out[me] = picks[me]
    rows.start()
    gather.run(first=False)
    rows.wait_recv()
    rows.wait_send()
    table.wait_send()
    for copy in own:
        copy.wait()


def gather_weights(small, num_tokens, embed, attn_w, fc1_w, fc2_w):
    lanes = 128
    body = embed.shape[0] // lanes * lanes
    tail = jnp.zeros((lanes, embed.shape[1]), embed.dtype).at[:embed.shape[0] - body].set(embed[body:])
    def whole(array, dim):
        return jax.ShapeDtypeStruct(array.shape[:dim] + (array.shape[dim] * NUM_DEV,) + array.shape[dim + 1:], array.dtype)

    any_spec = pl.BlockSpec(memory_space=pl.ANY)
    vmem = pl.BlockSpec(memory_space=pltpu.VMEM)
    num_layers = attn_w.shape[0]
    width = embed.shape[1]
    dma = pltpu.SemaphoreType.DMA
    return pl.pallas_call(
        weights_kernel,
        out_shape=(jax.ShapeDtypeStruct((NUM_DEV,) + small.shape, jnp.float32), jax.ShapeDtypeStruct((NUM_DEV, SLOTS, width), embed.dtype),
                   whole(attn_w, 2), whole(fc1_w, 1), whole(fc2_w, 1)),
        in_specs=[vmem] * 2 + [any_spec] * 4,
        out_specs=(vmem, vmem) + (any_spec,) * 3,
        scratch_shapes=[
            pltpu.VMEM((NUM_DEV + 8, num_tokens), jnp.float32), pltpu.VMEM((NUM_DEV + 8, num_tokens), jnp.float32),
            pltpu.VMEM((NUM_DEV * SLOTS, body + lanes), jnp.bfloat16), pltpu.VMEM((NUM_DEV, SLOTS, width), jnp.bfloat16), pltpu.VMEM((body + lanes, width), jnp.bfloat16),
            dma((num_layers, 5, 16, len(WAYS))), dma((num_layers, 5, NUM_DEV)), dma((4,)),
            dma((NUM_DEV,)), dma((NUM_DEV,)), dma((NUM_DEV,)), dma((NUM_DEV,)),
        ],
        compiler_params=pltpu.CompilerParams(collective_id=1, has_side_effects=True, vmem_limit_bytes=40 * 1024 * 1024),
        cost_estimate=pl.CostEstimate(flops=200_000_000_000, bytes_accessed=120_000_000, transcendentals=0),
        name='gather_weights',
    )(small, tail, embed, attn_w, fc1_w, fc2_w)


def rows_kernel(in_ref, out_ref, send_sem, recv_sem, own_sem):
    grid = Grid()
    share = in_ref.shape[1]
    half = share // 2

    def piece(step, part, order):
        return (in_ref.at[step, pl.ds(part * half, half)],
                lambda source: out_ref.at[step, pl.ds(pl.multiple_of(share * source + part * half, half), half)], order)

    own = pltpu.make_async_copy(in_ref, out_ref.at[:, pl.ds(pl.multiple_of(share * grid.me, share), share)], own_sem)
    own.start()
    grid.neighbour_barrier()
    Gather(grid, lambda wave: [piece(0, 0, 'xzy'), piece(0, 1, 'yzx'), piece(1, 0, ORDER_A), piece(1, 1, ORDER_B)], 1, send_sem, recv_sem).run()
    own.wait()


def gather_rows(rows):
    steps, share, width = rows.shape
    vmem = pl.BlockSpec(memory_space=pltpu.VMEM)
    return pl.pallas_call(
        rows_kernel,
        out_shape=jax.ShapeDtypeStruct((steps, share * 32, width), rows.dtype),
        in_specs=[vmem],
        out_specs=vmem,
        scratch_shapes=[pltpu.SemaphoreType.DMA((1, 4, 16, len(WAYS))), pltpu.SemaphoreType.DMA((1, 4, 32)), pltpu.SemaphoreType.DMA],
        compiler_params=pltpu.CompilerParams(collective_id=2, has_side_effects=True),
        cost_estimate=pl.CostEstimate(flops=20_000_000_000, bytes_accessed=8_000_000, transcendentals=0),
        name='gather_rows',
    )(rows)


def norm_rows(values, gain_row, shift_row):
    row_mean = jnp.mean(values, axis=-1, keepdims=True)
    centered = values - row_mean
    variance = jnp.mean(centered * centered, axis=-1, keepdims=True)
    return centered * lax.rsqrt(variance + LN_EPS) * gain_row + shift_row


UNROLL = 4


def layers_kernel(pos_ref, len_ref, tok_ref, posrow_ref, embnorm_ref, table_ref, fc1b_ref, attn_hbm, fc1_hbm, fc2_hbm,
                  self_k_hbm, self_v_hbm, cross_k_hbm, cross_v_hbm, rows_ref, out_k_hbm, out_v_hbm,
                  attn_buf, fc1_buf, fc2_buf, kbuf, vbuf, ckbuf, cvbuf, q3, k3, v3, o3, xs, inner, w_sem, c_sem, o_sem):
    num_layers, num_rows, num_times, num_heads, head_dim = kbuf.shape
    num_steps = xs.shape[0] // num_rows
    width = xs.shape[1]
    fat = num_steps * num_heads

    def weight_copy(layer, which):
        if which < 6:
            return pltpu.make_async_copy(attn_hbm.at[layer, which], attn_buf.at[which], w_sem.at[which])
        if which == 6:
            return pltpu.make_async_copy(fc1_hbm.at[layer], fc1_buf, w_sem.at[6])
        return pltpu.make_async_copy(fc2_hbm.at[layer], fc2_buf, w_sem.at[7])

    def self_copy(layer):
        return (pltpu.make_async_copy(self_k_hbm.at[layer], kbuf.at[layer], c_sem.at[0, layer]),
                pltpu.make_async_copy(self_v_hbm.at[layer], vbuf.at[layer], c_sem.at[1, layer]))

    def cross_copy(layer):
        return (pltpu.make_async_copy(cross_k_hbm.at[layer], ckbuf, c_sem.at[2, 0]),
                pltpu.make_async_copy(cross_v_hbm.at[layer], cvbuf, c_sem.at[2, 1]))

    def out_copy(layer):
        return (pltpu.make_async_copy(kbuf.at[layer], out_k_hbm.at[layer], o_sem.at[0, layer]),
                pltpu.make_async_copy(vbuf.at[layer], out_v_hbm.at[layer], o_sem.at[1, layer]))

    for which in (0, 1, 2):
        weight_copy(0, which).start()
    for copy in self_copy(0):
        copy.start()
    for which in (3, 4):
        weight_copy(0, which).start()
    for copy in cross_copy(0):
        copy.start()
    for which in (5, 6, 7):
        weight_copy(0, which).start()
    for layer in range(1, num_layers):
        for copy in self_copy(layer):
            copy.start()

    gain = embnorm_ref[pl.ds(0, 1), :].astype(jnp.float32)
    shift = embnorm_ref[pl.ds(1, 1), :].astype(jnp.float32)
    xs[...] = norm_rows(tok_ref[...].astype(jnp.float32) + posrow_ref[...].astype(jnp.float32), gain, shift)

    row_id = lax.broadcasted_iota(jnp.int32, (fat, num_times * num_heads), 0)
    col_id = lax.broadcasted_iota(jnp.int32, (fat, num_times * num_heads), 1)
    same_head = lax.rem(row_id, num_heads) == lax.rem(col_id, num_heads)
    step_id, time_id = row_id // num_heads, col_id // num_heads
    self_rank = jnp.where(same_head, time_id - step_id, num_times * 2)
    cross_rank = jnp.where(same_head, time_id, num_times * 2)

    def row(index):
        return table_ref[pl.ds(index, 1), :]

    def project(values, which, layer):
        out = jnp.dot(values, attn_buf[which], preferred_element_type=jnp.float32) + row(layer * 6 + which)
        return out

    def refill(layer, which):
        @pl.when(layer + 1 < num_layers)
        def _():
            weight_copy(layer + 1, which).start()

    def split_heads(values, ref):
        for head in range(num_heads):
            ref[:, head, :] = values[:, head * head_dim:(head + 1) * head_dim]

    def join_heads(ref):
        return jnp.concatenate([ref[:, head, :] for head in range(num_heads)], axis=1)

    def per_step(ref, index):
        return jnp.concatenate([ref[step * num_rows + index] for step in range(num_steps)], axis=0)

    def attend_one(index, keys, vals, rank, last):
        query = per_step(q3, index).astype(jnp.bfloat16)
        keys = keys.reshape(num_times * num_heads, head_dim)
        vals = vals.reshape(num_times * num_heads, head_dim)
        scores = lax.dot_general(query, keys, (((1,), (1,)), ((), ())), preferred_element_type=jnp.float32)
        scores = jnp.where(rank <= last, scores, -jnp.inf)
        weights = jnp.exp(scores - jnp.max(scores, axis=-1, keepdims=True))
        total = jnp.sum(weights, axis=-1, keepdims=True)
        mixed = jnp.dot(weights.astype(jnp.bfloat16), vals, preferred_element_type=jnp.float32) / total
        for step in range(num_steps):
            o3[step * num_rows + index] = mixed[step * num_heads:(step + 1) * num_heads]

    def layer_body(layer, carry):
        scale = head_dim ** -0.5
        act = xs[...].astype(jnp.bfloat16)
        for which, ref in ((0, q3), (1, k3), (2, v3)):
            weight_copy(layer, which).wait()
            out = project(act, which, layer)
            split_heads(out * scale if which == 0 else out, ref)
            refill(layer, which)
        for copy in self_copy(layer):
            copy.wait()

        def self_group(group, carry):
            for lane in range(UNROLL):
                index = group * UNROLL + lane
                pos = pos_ref[index]
                for step in range(num_steps):
                    kbuf[layer, index, pos + step] = k3[step * num_rows + index].astype(jnp.bfloat16)
                    vbuf[layer, index, pos + step] = v3[step * num_rows + index].astype(jnp.bfloat16)
                attend_one(index, kbuf[layer, index], vbuf[layer, index], self_rank, pos)
            return carry

        lax.fori_loop(0, num_rows // UNROLL, self_group, 0)
        for copy in out_copy(layer):
            copy.start()
        weight_copy(layer, 3).wait()
        mixed = join_heads(o3).astype(jnp.bfloat16)
        out = project(mixed, 3, layer)
        refill(layer, 3)
        xs[...] = norm_rows(xs[...] + out, row(ROW_GAIN + layer * 3), row(ROW_SHIFT + layer * 3))

        weight_copy(layer, 4).wait()
        split_heads(project(xs[...].astype(jnp.bfloat16), 4, layer) * scale, q3)
        refill(layer, 4)
        for copy in cross_copy(layer):
            copy.wait()

        def cross_group(group, carry):
            for lane in range(UNROLL):
                index = group * UNROLL + lane
                attend_one(index, ckbuf[index], cvbuf[index], cross_rank, len_ref[index] - 1)
            return carry

        lax.fori_loop(0, num_rows // UNROLL, cross_group, 0)

        @pl.when(layer + 1 < num_layers)
        def _():
            for copy in cross_copy(layer + 1):
                copy.start()

        weight_copy(layer, 5).wait()
        mixed = join_heads(o3).astype(jnp.bfloat16)
        out = project(mixed, 5, layer)
        refill(layer, 5)
        xs[...] = norm_rows(xs[...] + out, row(ROW_GAIN + layer * 3 + 1), row(ROW_SHIFT + layer * 3 + 1))

        weight_copy(layer, 6).wait()
        act = xs[...].astype(jnp.bfloat16)
        tile = 512

        def up_tile(index, carry):
            cols = pl.ds(pl.multiple_of(index * tile, tile), tile)
            out = jnp.dot(act, fc1_buf[:, cols], preferred_element_type=jnp.float32) + fc1b_ref[pl.ds(layer, 1), cols]
            inner[:, cols] = (0.5 * out * (1.0 + lax.erf(out * (2.0 ** -0.5)))).astype(jnp.bfloat16)
            return carry

        lax.fori_loop(0, fc1_buf.shape[1] // tile, up_tile, 0)
        refill(layer, 6)
        weight_copy(layer, 7).wait()

        def down_tile(index, total):
            cols = pl.ds(pl.multiple_of(index * tile, tile), tile)
            return total + jnp.dot(inner[:, cols], fc2_buf[cols, :], preferred_element_type=jnp.float32)

        out = lax.fori_loop(0, fc2_buf.shape[0] // tile, down_tile, jnp.zeros(xs.shape, jnp.float32)) + row(ROW_FC2 + layer)
        refill(layer, 7)
        xs[...] = norm_rows(xs[...] + out, row(ROW_GAIN + layer * 3 + 2), row(ROW_SHIFT + layer * 3 + 2))
        return carry

    lax.fori_loop(0, num_layers, layer_body, 0)
    rows_ref[...] = xs[...].astype(jnp.bfloat16)
    for layer in range(num_layers):
        for copy in out_copy(layer):
            copy.wait()


def run_layers(positions, src_len, tok_rows, pos_rows, emb_norm, table, fc1_b, attn_full, fc1_full, fc2_full, self_k, self_v, cross_k, cross_v):
    smem = pl.BlockSpec(memory_space=pltpu.SMEM)
    vmem = pl.BlockSpec(memory_space=pltpu.VMEM)
    any_spec = pl.BlockSpec(memory_space=pl.ANY)
    num_tok, width = tok_rows.shape
    heads, dim = self_k.shape[3:]
    bf16, f32 = jnp.bfloat16, jnp.float32
    return pl.pallas_call(
        layers_kernel,
        out_shape=(jax.ShapeDtypeStruct((num_tok, width), bf16), jax.ShapeDtypeStruct(self_k.shape, bf16), jax.ShapeDtypeStruct(self_v.shape, bf16)),
        in_specs=[smem, smem] + [vmem] * 5 + [any_spec] * 7,
        out_specs=(vmem, any_spec, any_spec),
        scratch_shapes=[
            pltpu.VMEM(attn_full.shape[1:], bf16), pltpu.VMEM(fc1_full.shape[1:], bf16), pltpu.VMEM(fc2_full.shape[1:], bf16),
            pltpu.VMEM(self_k.shape, bf16), pltpu.VMEM(self_v.shape, bf16), pltpu.VMEM(cross_k.shape[1:], bf16), pltpu.VMEM(cross_v.shape[1:], bf16),
            pltpu.VMEM((num_tok, heads, dim), f32), pltpu.VMEM((num_tok, heads, dim), f32), pltpu.VMEM((num_tok, heads, dim), f32), pltpu.VMEM((num_tok, heads, dim), f32),
            pltpu.VMEM((num_tok, width), f32), pltpu.VMEM((num_tok, fc1_full.shape[2]), bf16),
            pltpu.SemaphoreType.DMA((8,)), pltpu.SemaphoreType.DMA((3, 2)), pltpu.SemaphoreType.DMA((2, 2)),
        ],
        compiler_params=pltpu.CompilerParams(vmem_limit_bytes=63 * 1024 * 1024),
        cost_estimate=pl.CostEstimate(flops=8_000_000_000, bytes_accessed=110_000_000, transcendentals=4_000_000),
        name='run_layers',
    )(positions, src_len, tok_rows, pos_rows, emb_norm, table, fc1_b, attn_full, fc1_full, fc2_full, self_k, self_v, cross_k, cross_v)


def logits_kernel(emb_ref, rows_ref, bias_ref, out_ref):
    steps, num_rows, _ = rows_ref.shape
    block = emb_ref.shape[0]
    lanes = 128
    stride = steps * num_rows // lanes
    for step in range(steps):
        scores = lax.dot_general(emb_ref[...], rows_ref[step], (((1,), (1,)), ((), ())), preferred_element_type=jnp.float32) + bias_ref[...]
        for part in range(num_rows // lanes):
            out_ref[pl.ds(part * steps + step, block, stride=stride), :] = scores[:, part * lanes:(part + 1) * lanes]


def run_logits(tok_embed, all_rows, bias):
    vocab, width = tok_embed.shape
    steps, num_rows, _ = all_rows.shape
    block = 528
    per = steps * num_rows // 128
    out = pl.pallas_call(
        logits_kernel,
        grid=(pl.cdiv(vocab, block),),
        out_shape=jax.ShapeDtypeStruct((vocab * per, 128), jnp.float32),
        in_specs=[pl.BlockSpec((block, width), lambda i: (i, 0)), pl.BlockSpec((steps, num_rows, width), lambda i: (0, 0, 0)), pl.BlockSpec((block, 1), lambda i: (i, 0))],
        out_specs=pl.BlockSpec((block * per, 128), lambda i: (i, 0)),
        compiler_params=pltpu.CompilerParams(dimension_semantics=('arbitrary',), vmem_limit_bytes=67_043_328),
        cost_estimate=pl.CostEstimate(flops=2 * vocab * width * steps * num_rows, bytes_accessed=20_000_000, transcendentals=0),
        name='run_logits',
    )(tok_embed, all_rows, bias[:, None])
    return out.reshape(vocab, num_rows // 128, steps, 128).transpose(2, 1, 3, 0).reshape(steps, num_rows, vocab)


def solution(mesh):
    cache_spec = P(None, 'fsdp')
    in_specs = (P('fsdp'), P('fsdp'), P('fsdp'), cache_spec, cache_spec, cache_spec, cache_spec,
                P(None, None, 'fsdp'), P(None, None, 'fsdp'), P(None, 'fsdp'), P(None, 'fsdp'),
                P(None, 'fsdp'), P(None, 'fsdp'), P(None, None, 'fsdp'), P(None, None, 'fsdp'),
                P('fsdp'), P(), P(), P('fsdp'))
    out_specs = (P(None, None, 'fsdp'), cache_spec, cache_spec)

    def local_decode(tokens, positions, src_len, self_k, self_v, cross_k, cross_v, attn_w, attn_b, fc1_w, fc1_b, fc2_w, fc2_b, ln_gain, ln_bias, tok_embed, pos_embed, emb_norm, logit_bias):
        shard_idx = lax.axis_index('fsdp')
        num_layers = attn_w.shape[0]
        num_rows, num_steps = tokens.shape
        vocab_local, width = tok_embed.shape
        num_dev = mesh.shape['fsdp']
        small = (attn_b, fc2_b, ln_gain, ln_bias, tokens.T, fc1_b)
        packed = jnp.concatenate([part.astype(jnp.float32).reshape(-1, num_rows) for part in small], axis=0)
        gathered, found, attn_full, fc1_full, fc2_full = gather_weights(packed, num_steps * num_rows, tok_embed, attn_w, fc1_w, fc2_w)
        table = gathered.transpose(1, 0, 2).reshape(packed.shape[0], num_dev * num_rows)
        all_fc1_b = gathered[:, ROW_FC1:].reshape(num_dev, num_layers, -1).transpose(1, 0, 2).reshape(num_layers, -1)
        all_tokens = gathered[:, ROW_TOKEN:ROW_TOKEN + num_steps].astype(jnp.int32).reshape(num_dev, num_steps * num_rows)
        owner = all_tokens // vocab_local
        most = (owner[:, :, None] == jnp.arange(num_dev)).astype(jnp.int32).sum(axis=1).max()
        my_owner = (tokens.T // vocab_local).reshape(-1)
        order = jnp.arange(num_steps * num_rows)
        my_rank = ((my_owner[None, :] == my_owner[:, None]) & (order[None, :] < order[:, None])).astype(jnp.int32).sum(axis=1)

        def few(found):
            line = my_owner * SLOTS + my_rank
            chosen = (line[:, None] == jnp.arange(num_dev * SLOTS)).astype(found.dtype)
            return jnp.dot(chosen, found.reshape(num_dev * SLOTS, width), preferred_element_type=jnp.float32).astype(found.dtype)

        def many(found):
            local = all_tokens - shard_idx * vocab_local
            mine = (local >= 0) & (local < vocab_local)
            rows = jnp.take(tok_embed, jnp.clip(local, 0, vocab_local - 1), axis=0)
            rows = jnp.where(mine[:, :, None], rows, jnp.zeros_like(rows))
            rows = lax.all_to_all(rows, 'fsdp', 0, 0)
            return rows.astype(jnp.float32).sum(axis=0).astype(found.dtype)

        tok_rows = lax.cond(most > SLOTS, many, few, found)
        step_pos = positions[None, :] + jnp.arange(num_steps)[:, None]
        pos_rows = jnp.take(pos_embed, step_pos + 2, axis=0).reshape(num_steps * num_rows, width)
        rows, cache_k, cache_v = run_layers(positions, src_len, tok_rows, pos_rows, emb_norm, table, all_fc1_b, attn_full, fc1_full, fc2_full, self_k, self_v, cross_k, cross_v)
        all_rows = gather_rows(rows.reshape(num_steps, num_rows, width))
        return run_logits(tok_embed, all_rows, logit_bias), cache_k, cache_v

    return jax.shard_map(local_decode, mesh=mesh, in_specs=in_specs, out_specs=out_specs, check_vma=False)
```
